32 devices in a mesh: row: 4 (over y, core), col: 8 (over z, x).
Axes of the slice: x: 2, y: 2, z: 4, core: 2. Of those that a mesh axis runs over, the one named last changes fastest.
Arguments:
- volume: float32 [8, 1024, 1024], P(None, 'row', 'col'), may hold values from -6 to 6
- ray_weights: float32 [16, 1024], P(None, 'row'), may hold values from 0.5 to 2
- shear_weights: bfloat16 [16, 128, 128], replicated, may hold values from -0.5 to 0.5
- shear_offsets: int32 [16], replicated, may hold values from 0 to 7
- measured: float32 [16, 8, 1024], P('row', None, 'col'), may hold values from -6 to 6
Outputs:
- residual: float32 [16, 8, 1024], P('row', None, 'col')
- gradient: float32 [8, 1024, 1024], P(None, 'row', 'col')
The draws below stay inside these ranges and needn't reach their ends.
All inputs are finite; a program needn't handle non-finite values.
Results may differ from the reference program's by a relative error of at most 0.0003.
Values sent between devices are 32-bit elements; how exact they have to be, the bound alone decides.
A program may use at most 64 MiB of HBM per device.

```python
import math
import jax
import jax.numpy as jnp
from jax import lax

CX = 256
CY = 128
SL = 8
NX = 1024
NY = 1024
ANGLES = 16
N_ROW = 4
N_COL = 8


def plant(values, key, smallest, high):
    extent = values.shape
    index_at = [jax.random.randint(jax.random.fold_in(key, axis), (), 0, extent[axis]) for axis in range(len(extent))]
    values = values.at[tuple(index_at)].set(smallest)
    longest = extent.index(max(extent))
    index_at[longest] = (index_at[longest] + 1) % extent[longest]
    return values.at[tuple(index_at)].set(high)


def steps_of(rng, dims, shards, smallest, high):
    factor_of, own = 1.0, jax.random.fold_in(rng, 6)
    for axis_at, parts in shards:
        heights = jnp.exp(jax.random.uniform(jax.random.fold_in(own, axis_at), (parts,), jnp.float32, smallest / len(shards), high / len(shards)))
        factor_of = factor_of * jnp.repeat(heights, dims[axis_at] // parts).reshape([-1 if axis == axis_at else 1 for axis in range(len(dims))])
    return factor_of


def noise(stream_key, dims, scale, bound, pieces=(), kind=jnp.bfloat16):
    array = scale * jax.random.normal(stream_key, dims, jnp.float32)
    if pieces:
        array = array * steps_of(stream_key, dims, pieces, -0.22, 0.18)
    return jnp.clip(array, -bound, bound).astype(kind)


def setup_inputs(seed: int = 0) -> dict:
    streams_of = jax.random.split(jax.random.key(seed), 6)
    volume = noise(streams_of[0], (SL, NX, NY), 1.0, 6.0, ((1, 4), (2, 8)), jnp.float32)
    ray_weights = jnp.clip(jnp.exp(math.log(2.0) - 1.3862944 * jax.random.uniform(streams_of[1], (ANGLES, NX), jnp.float32) ** steps_of(streams_of[1], (ANGLES, NX), ((1, 4),), -0.2, 0.2)), 0.5, 2.0)
    shear_weights = noise(streams_of[2], (ANGLES, CY, CY), CY ** -0.5, 0.5)
    shear_offsets = plant(jax.random.randint(streams_of[3], (ANGLES,), 0, N_COL), jax.random.fold_in(streams_of[3], 1), 0, N_COL - 1).astype(jnp.int32)
    measured = noise(streams_of[4], (ANGLES, SL, NY), 1.0, 6.0, ((0, 4), (2, 8)), jnp.float32)
    return dict(volume=volume, ray_weights=ray_weights, shear_weights=shear_weights, shear_offsets=shear_offsets, measured=measured)


def reference(volume, ray_weights, shear_weights, shear_offsets, measured):
    highest = lax.Precision.HIGHEST
    factor = 1.0 / math.sqrt(NX)
    blocks = volume.reshape(SL, N_ROW, CX, NY)
    weights_rows = ray_weights.reshape(ANGLES, N_ROW, CX)
    tilesum = jnp.einsum('arx,srxn->arsn', weights_rows, blocks, precision=highest) * factor
    shear = shear_weights.astype(jnp.float32)
    tiles = tilesum.reshape(ANGLES, N_ROW, SL, N_COL, CY)
    projected = jnp.einsum('arscy,ayz->arscz', tiles, shear, precision=highest)
    row_positions = jnp.arange(N_ROW, dtype=jnp.int32)
    col_positions = jnp.arange(N_COL, dtype=jnp.int32)
    moved = shear_offsets.astype(jnp.int32)[:, None, None] * row_positions[None, :, None]
    source = (col_positions[None, None, :] - moved) % N_COL
    full_shape = (ANGLES, N_ROW, SL, N_COL, CY)
    source_index = jnp.broadcast_to(source[:, :, None, :, None], full_shape).astype(jnp.int32)
    landed = jnp.take_along_axis(projected, source_index, axis=3)
    projection = lax.optimization_barrier(jnp.sum(landed, axis=1)).reshape(ANGLES, SL, NY)
    residual = projection - measured
    target = (col_positions[None, None, :] + moved) % N_COL
    target_index = jnp.broadcast_to(target[:, :, None, :, None], full_shape).astype(jnp.int32)
    resid_tiles = jnp.broadcast_to(residual.reshape(ANGLES, 1, SL, N_COL, CY), full_shape)
    pulled = jnp.take_along_axis(resid_tiles, target_index, axis=3)
    spread = jnp.einsum('arscz,ayz->arscy', pulled, shear, precision=highest)
    spread = spread.reshape(ANGLES, N_ROW, SL, NY)
    gradient = jnp.einsum('arx,arsn->srxn', weights_rows, spread, precision=highest) * factor
    return (residual, gradient.reshape(SL, NX, NY))
```

```python
import functools
import math

import jax
import jax.numpy as jnp
from jax import lax
from jax.experimental import pallas as pl
from jax.experimental.pallas import tpu as pltpu
from jax.sharding import PartitionSpec as P

MESH = pl.DeviceIdType.MESH
UNROLL_UP_TO = 64


def split(value):
    high = value.astype(jnp.bfloat16)
    return high, (value - high.astype(jnp.float32)).astype(jnp.bfloat16)


def each(count, body):
    if count <= UNROLL_UP_TO:
        for step in range(count):
            body(step)
    else:
        lax.fori_loop(0, count, lambda step, _: (body(step), 0)[1], 0)


def bytes_of(ref, blocks, sem):
    part = ref.at[pl.ds(0, blocks)]
    return pltpu.make_async_copy(part, part, sem)


def kernel(
    rows, cols, factor,
    volume_ref, weights_ref, shear_ref, offsets_ref, measured_ref,
    residual_ref, gradient_ref,
    slab, shear, tiles, sends, landed, measure_out, measure_in, resid, pulls, pulled, resid_in,
    slab_sem, shear_sem, out_sem, in_sem, back_out_sem, back_in_sem, m_out_sem, m_in_sem, r_out_sem, r_in_sem,
):
    slices = volume_ref.shape[0]
    angles = weights_ref.shape[0]
    unit = landed.shape[1]
    pieces = slices // unit
    count = rows * cols
    row, col = lax.axis_index("row"), lax.axis_index("col")
    me = row * cols + col

    def peer(step):
        other = lax.rem(me + step + 1, count)
        return other, (other // cols, lax.rem(other, cols))

    def mate(step):
        other = lax.rem(col + step + 1, cols)
        return other, (row, other)

    volume_copies = []
    for s in range(slices):
        copy = pltpu.make_async_copy(volume_ref.at[s], slab.at[s], slab_sem.at[s])
        copy.start()
        volume_copies.append(copy)
    shear_copy = pltpu.make_async_copy(shear_ref, shear, shear_sem)
    shear_copy.start()

    barrier = pltpu.get_barrier_semaphore()
    each(count - 1, lambda step: pl.semaphore_signal(barrier, inc=1, device_id=peer(step)[1], device_id_type=MESH))

    for m in range(cols):
        angle, first = (m * unit) // slices, (m * unit) % slices
        measure_out[m] = measured_ref[angle, first:first + unit, :]

    weights = weights_ref[...] * factor
    w_high, w_low = split(weights)
    w_both = jnp.concatenate([w_high, w_low], axis=0)
    for s in range(slices):
        volume_copies[s].wait()
        v_high, v_low = split(slab[s])
        first = jnp.dot(w_both, v_high, preferred_element_type=jnp.float32)
        second = jnp.dot(w_high, v_low, preferred_element_type=jnp.float32)
        tiles[pl.ds(s, angles, stride=slices), :] = first[:angles] + first[angles:] + second
    shear_copy.wait()
    for a in range(angles):
        t_high, t_low = split(tiles[a * slices:(a + 1) * slices, :])
        both = jnp.dot(jnp.concatenate([t_high, t_low], axis=0), shear[a], preferred_element_type=jnp.float32)
        done = both[:slices] + both[slices:]
        for h in range(pieces):
            sends[a * pieces + h] = done[h * unit:(h + 1) * unit]

    pl.semaphore_wait(barrier, count - 1)

    def send_measured(step):
        other, device = mate(step)
        pltpu.make_async_remote_copy(
            src_ref=measure_out.at[other], dst_ref=measure_in.at[col], send_sem=m_out_sem, recv_sem=m_in_sem,
            device_id=device, device_id_type=MESH).start()

    def send_tile(step):
        other, device = peer(step)
        pltpu.make_async_remote_copy(
            src_ref=sends.at[other], dst_ref=landed.at[me], send_sem=out_sem, recv_sem=in_sem,
            device_id=device, device_id_type=MESH).start()

    each(cols - 1, send_measured)
    each(count - 1, send_tile)
    landed[me] = sends[me]
    measure_in[col] = measure_out[col]
    w_columns = jnp.concatenate([weights, weights - w_high.astype(jnp.float32), weights], axis=0).T.astype(jnp.bfloat16)
    offset = offsets_ref[me // pieces]
    bytes_of(measure_in, cols - 1, m_in_sem).wait()
    bytes_of(landed, count - 1, in_sem).wait()

    for c in range(cols):
        total = landed[c]
        for r in range(1, rows):
            total = total + landed[r * cols + lax.rem((cols - offset) * r + c, cols)]
        resid[c] = total - measure_in[c]

    for r in range(rows):
        for c in range(cols):
            pulls[r * cols + c] = resid[lax.rem(offset * r + c, cols)]

    def send_pull(step):
        other, device = peer(step)
        pltpu.make_async_remote_copy(
            src_ref=pulls.at[other], dst_ref=pulled.at[me], send_sem=back_out_sem, recv_sem=back_in_sem,
            device_id=device, device_id_type=MESH).start()

    def send_resid(step):
        other, device = mate(step)
        pltpu.make_async_remote_copy(
            src_ref=resid.at[other], dst_ref=resid_in.at[col], send_sem=r_out_sem, recv_sem=r_in_sem,
            device_id=device, device_id_type=MESH).start()

    each(count - 1, send_pull)
    each(cols - 1, send_resid)
    pulled[me] = pulls[me]
    resid_in[col] = resid[col]
    bytes_of(pulled, count - 1, back_in_sem).wait()

    for a in range(angles):
        value = jnp.concatenate([pulled[a * pieces + h] for h in range(pieces)], axis=0)
        p_high, p_low = split(value)
        both = lax.dot_general(
            jnp.concatenate([p_high, p_low], axis=0), shear[a], (((1,), (1,)), ((), ())),
            preferred_element_type=jnp.float32)
        tiles[a * slices:(a + 1) * slices, :] = both[:slices] + both[slices:]
    for s in range(slices):
        g_high, g_low = split(tiles[pl.ds(s, angles, stride=slices), :])
        gradient_ref[s] = jnp.dot(
            w_columns, jnp.concatenate([g_high, g_high, g_low], axis=0), preferred_element_type=jnp.float32)

    bytes_of(resid_in, cols - 1, r_in_sem).wait()
    for m in range(cols):
        angle, first = (m * unit) // slices, (m * unit) % slices
        residual_ref[angle, first:first + unit, :] = resid_in[m]
    bytes_of(measure_out, cols - 1, m_out_sem).wait()
    bytes_of(sends, count - 1, out_sem).wait()
    bytes_of(pulls, count - 1, back_out_sem).wait()
    bytes_of(resid, cols - 1, r_out_sem).wait()


def on_device(volume, ray_weights, shear_weights, shear_offsets, measured):
    rows, cols = lax.axis_size("row"), lax.axis_size("col")
    slices, slab_rows, width = volume.shape
    angles = ray_weights.shape[0]
    unit = measured.shape[0] * slices // cols
    count = rows * cols
    f32 = jnp.float32
    blocks = pltpu.VMEM((count, unit, width), f32)
    few = pltpu.VMEM((cols, unit, width), f32)
    dma = pltpu.SemaphoreType.DMA
    vmem = pl.BlockSpec(memory_space=pltpu.VMEM)
    return pl.pallas_call(
        functools.partial(kernel, rows, cols, 1.0 / math.sqrt(slab_rows * rows)),
        out_shape=(jax.ShapeDtypeStruct(measured.shape, f32), jax.ShapeDtypeStruct(volume.shape, f32)),
        in_specs=[
            pl.BlockSpec(memory_space=pl.ANY), vmem, pl.BlockSpec(memory_space=pl.ANY),
            pl.BlockSpec(memory_space=pltpu.SMEM), vmem],
        out_specs=(vmem, vmem),
        scratch_shapes=[
            pltpu.VMEM(volume.shape, f32),
            pltpu.VMEM(shear_weights.shape, shear_weights.dtype),
            pltpu.VMEM((angles * slices, width), f32),
            blocks, blocks, few, few, few, blocks, blocks, few,
            dma((slices,)), dma, dma, dma, dma, dma, dma, dma, dma, dma,
        ],
        compiler_params=pltpu.CompilerParams(collective_id=0, has_side_effects=True),
        name="project",
    )(volume, ray_weights, shear_weights, shear_offsets, measured)


def solution(mesh):
    placed = (P(None, "row", "col"), P(None, "row"), P(), P(), P("row", None, "col"))
    return jax.shard_map(
        on_device,
        mesh=mesh,
        in_specs=placed,
        out_specs=(P("row", None, "col"), P(None, "row", "col")),
        check_vma=False,
    )
```

```python
import functools
import math

import jax
import jax.numpy as jnp
from jax import lax
from jax.experimental import pallas as pl
from jax.experimental.pallas import tpu as pltpu
from jax.sharding import PartitionSpec as P

MESH = pl.DeviceIdType.MESH
UNROLL_UP_TO = 64
KERNEL_VMEM = 24 * 1024 * 1024


def split(value):
    high = value.astype(jnp.bfloat16)
    return high, (value - high.astype(jnp.float32)).astype(jnp.bfloat16)


def each(count, body):
    if count <= UNROLL_UP_TO:
        for step in range(count):
            body(step)
    else:
        lax.fori_loop(0, count, lambda step, _: (body(step), 0)[1], 0)


def bytes_of(ref, blocks, sem):
    part = ref.at[pl.ds(0, blocks)]
    return pltpu.make_async_copy(part, part, sem)


def exchange(
    rows, cols, factor,
    volume_ref, weights_ref, shear_ref, offsets_ref, measured_ref,
    columns_ref, spread_ref, residual_ref,
    slab, weights_in, shear, offsets, measured, sums, tiles, landed, measure_in, resid, pulls, pulled, resid_in,
    slab_sem, local_sem, out_sem, in_sem, back_out_sem, back_in_sem, m_out_sem, m_in_sem, r_out_sem, r_in_sem,
):
    slices = volume_ref.shape[0]
    angles = weights_ref.shape[0]
    owned = measured_ref.shape[0]
    base = (cols - owned) // 2
    count = rows * cols
    row, col = lax.axis_index("row"), lax.axis_index("col")
    me = row * cols + col
    at_home = jnp.logical_and(col >= base, col < base + owned)
    away = jnp.logical_not(at_home)
    mine = row * owned + lax.clamp(0, col - base, owned - 1)

    def home(angle):
        return angle // owned, base + lax.rem(angle, owned)

    def peer(step):
        other = lax.rem(me + step + 1, count)
        return other, (other // cols, lax.rem(other, cols))

    def signal(device):
        pl.semaphore_signal(barrier, inc=1, device_id=device, device_id_type=MESH)

    weights_copy = pltpu.make_async_copy(weights_ref, weights_in, local_sem.at[0])
    weights_copy.start()
    volume_copies = []
    for s in range(slices):
        copy = pltpu.make_async_copy(volume_ref.at[s], slab.at[s], slab_sem.at[s])
        copy.start()
        volume_copies.append(copy)
    shear_copy = pltpu.make_async_copy(shear_ref, shear, local_sem.at[1])
    shear_copy.start()
    measured_copy = pltpu.make_async_copy(measured_ref, measured, local_sem.at[2])
    measured_copy.start()
    offsets_copy = pltpu.make_async_copy(offsets_ref, offsets, local_sem.at[3])
    offsets_copy.start()

    barrier = pltpu.get_barrier_semaphore()

    @pl.when(at_home)
    def _():
        each(count - 1, lambda step: signal(peer(step)[1]))

    @pl.when(away)
    def _():
        each(angles, lambda angle: signal(home(angle)))

    weights_copy.wait()
    weights = weights_in[...] * factor
    w_high, w_low = split(weights)
    w_both = jnp.concatenate([w_high, w_low], axis=0)
    for s in range(slices):
        volume_copies[s].wait()
        v_high, v_low = split(slab[s])
        first = jnp.dot(w_both, v_high, preferred_element_type=jnp.float32)
        second = jnp.dot(w_high, v_low, preferred_element_type=jnp.float32)
        sums[pl.ds(s, angles, stride=slices), :] = first[:angles] + first[angles:] + second
    shear_copy.wait()
    for a in range(angles):
        t_high, t_low = split(sums[a * slices:(a + 1) * slices, :])
        both = jnp.dot(jnp.concatenate([t_high, t_low], axis=0), shear[a], preferred_element_type=jnp.float32)
        tiles[a] = both[:slices] + both[slices:]
    measured_copy.wait()
    offsets_copy.wait()

    @pl.when(at_home)
    def _():
        pl.semaphore_wait(barrier, count - 1)

    @pl.when(away)
    def _():
        pl.semaphore_wait(barrier, angles)

    def send(source, target, send_sem, recv_sem, device):
        pltpu.make_async_remote_copy(
            src_ref=source, dst_ref=target, send_sem=send_sem, recv_sem=recv_sem,
            device_id=device, device_id_type=MESH).start()

    def send_measured(step):
        place = lax.rem(lax.select(at_home, col - base + 1, 0) + step, owned)
        send(measured.at[place], measure_in.at[col], m_out_sem, m_in_sem, (row, base + place))

    def send_tile(step):
        angle = lax.rem(lax.select(at_home, mine + 1, row * owned) + step, angles)
        send(tiles.at[angle], landed.at[me], out_sem, in_sem, home(angle))

    each(angles - 1, send_tile)

    @pl.when(away)
    def _():
        send_tile(angles - 1)

    each(owned - 1, send_measured)

    @pl.when(away)
    def _():
        send_measured(owned - 1)

    columns_ref[...] = jnp.concatenate(
        [weights, weights - w_high.astype(jnp.float32), weights], axis=0).T.astype(jnp.bfloat16)

    @pl.when(at_home)
    def _():
        landed[me] = tiles[mine]
        measure_in[col] = measured[col - base]
        offset = offsets[mine]
        bytes_of(measure_in, cols - 1, m_in_sem).wait()
        bytes_of(landed, count - 1, in_sem).wait()
        for c in range(cols):
            total = landed[c]
            for r in range(1, rows):
                total = total + landed[r * cols + lax.rem((cols - offset) * r + c, cols)]
            resid[c] = total - measure_in[c]
        for r in range(rows):
            for c in range(cols):
                pulls[r * cols + c] = resid[lax.rem(offset * r + c, cols)]

        def send_pull(step):
            other, device = peer(step)
            send(pulls.at[other], pulled.at[mine], back_out_sem, back_in_sem, device)

        def send_resid(step):
            other = lax.rem(col + step + 1, cols)
            send(resid.at[other], resid_in.at[col - base], r_out_sem, r_in_sem, (row, other))

        each(count - 1, send_pull)
        each(cols - 1, send_resid)
        pulled[mine] = pulls[me]
        resid_in[col - base] = resid[col]
        bytes_of(pulled, angles - 1, back_in_sem).wait()

    @pl.when(away)
    def _():
        bytes_of(pulled, angles, back_in_sem).wait()

    for a in range(angles):
        p_high, p_low = split(pulled[a])
        both = lax.dot_general(
            jnp.concatenate([p_high, p_low], axis=0), shear[a], (((1,), (1,)), ((), ())),
            preferred_element_type=jnp.float32)
        sums[a * slices:(a + 1) * slices, :] = both[:slices] + both[slices:]
    for s in range(slices):
        g_high, g_low = split(sums[pl.ds(s, angles, stride=slices), :])
        spread_ref[s] = jnp.concatenate([g_high, g_high, g_low], axis=0)

    @pl.when(at_home)
    def _():
        bytes_of(resid_in, owned - 1, r_in_sem).wait()
        bytes_of(tiles, angles - 1, out_sem).wait()
        bytes_of(measured, owned - 1, m_out_sem).wait()
        bytes_of(pulls, count - 1, back_out_sem).wait()
        bytes_of(resid, cols - 1, r_out_sem).wait()

    @pl.when(away)
    def _():
        bytes_of(resid_in, owned, r_in_sem).wait()
        bytes_of(tiles, angles, out_sem).wait()
        bytes_of(measured, owned, m_out_sem).wait()

    residual_ref[...] = resid_in[...]


def finish(columns_ref, spread_ref, resid_ref, residual_ref, gradient_ref, stage, stage_sem, resid_sem):
    copies = [pltpu.make_async_copy(resid_ref, residual_ref, resid_sem)]
    copies[0].start()
    for s in range(spread_ref.shape[0]):
        stage[s] = jnp.dot(columns_ref[...], spread_ref[s], preferred_element_type=jnp.float32)
        copy = pltpu.make_async_copy(stage.at[s], gradient_ref.at[s], stage_sem.at[s])
        copy.start()
        copies.append(copy)
    for copy in copies:
        copy.wait()


def on_device(volume, ray_weights, shear_weights, shear_offsets, measured):
    rows, cols = lax.axis_size("row"), lax.axis_size("col")
    slices, slab_rows, width = volume.shape
    angles = ray_weights.shape[0]
    owned = measured.shape[0]
    count = rows * cols
    f32, bf16 = jnp.float32, jnp.bfloat16
    dma = pltpu.SemaphoreType.DMA
    vmem = pl.BlockSpec(memory_space=pltpu.VMEM)
    hbm = pl.BlockSpec(memory_space=pltpu.HBM)

    def blocks(number):
        return pltpu.VMEM((number, slices, width), f32)

    columns, spread, resid = pl.pallas_call(
        functools.partial(exchange, rows, cols, 1.0 / math.sqrt(slab_rows * rows)),
        out_shape=(
            jax.ShapeDtypeStruct((slab_rows, 3 * angles), bf16),
            jax.ShapeDtypeStruct((slices, 3 * angles, width), bf16),
            jax.ShapeDtypeStruct(measured.shape, f32)),
        in_specs=[hbm] * 5,
        out_specs=(vmem, vmem, vmem),
        scratch_shapes=[
            pltpu.VMEM(volume.shape, f32),
            pltpu.VMEM(ray_weights.shape, f32),
            pltpu.VMEM(shear_weights.shape, shear_weights.dtype),
            pltpu.SMEM(shear_offsets.shape, jnp.int32),
            blocks(owned),
            pltpu.VMEM((angles * slices, width), f32),
            blocks(angles), blocks(count), blocks(cols), blocks(cols), blocks(count), blocks(angles), blocks(owned),
            dma((slices,)), dma((4,)), dma, dma, dma, dma, dma, dma, dma, dma,
        ],
        compiler_params=pltpu.CompilerParams(collective_id=0, has_side_effects=True, vmem_limit_bytes=KERNEL_VMEM),
        name="exchange",
    )(*(pltpu.with_memory_space_constraint(value, pltpu.HBM)
        for value in (volume, ray_weights, shear_weights, shear_offsets, measured)))
    return pl.pallas_call(
        finish,
        out_shape=(jax.ShapeDtypeStruct(measured.shape, f32), jax.ShapeDtypeStruct(volume.shape, f32)),
        in_specs=[vmem] * 3,
        out_specs=(hbm, hbm),
        scratch_shapes=[pltpu.VMEM(volume.shape, f32), dma((slices,)), dma],
        compiler_params=pltpu.CompilerParams(vmem_limit_bytes=KERNEL_VMEM),
        name="finish",
    )(columns, spread, resid)


def solution(mesh):
    placed = (P(None, "row", "col"), P(None, "row"), P(), P(), P("row", None, "col"))
    return jax.shard_map(
        on_device,
        mesh=mesh,
        in_specs=placed,
        out_specs=(P("row", None, "col"), P(None, "row", "col")),
        check_vma=False,
    )
```

```python
import functools
import math

import jax
import jax.numpy as jnp
from jax import lax
from jax.experimental import pallas as pl
from jax.experimental.pallas import tpu as pltpu
from jax.sharding import PartitionSpec as P

MESH = pl.DeviceIdType.MESH
UNROLL_UP_TO = 64
KERNEL_VMEM = 24 * 1024 * 1024


def split(value):
    high = value.astype(jnp.bfloat16)
    return high, (value - high.astype(jnp.float32)).astype(jnp.bfloat16)


def each(count, body):
    if count <= UNROLL_UP_TO:
        for step in range(count):
            body(step)
    else:
        lax.fori_loop(0, count, lambda step, _: (body(step), 0)[1], 0)


def flip(index, step, size):
    if size & (size - 1):
        return lax.rem(index + step, size)
    bit = 1
    while bit < size:
        if step & bit:
            index = index + bit - 2 * bit * lax.rem(index // bit, 2)
        bit *= 2
    return index


def far_first(size):
    quarter = max(size // 4, 1)
    place = {2: 0, 3: 1, 1: 2, 0: 3}
    return sorted(range(size), key=lambda step: (place.get(step // quarter, 2), -step))


def bytes_of(ref, blocks, sem):
    part = ref.at[pl.ds(0, blocks)]
    return pltpu.make_async_copy(part, part, sem)


def exchange(
    rows, cols, factor,
    volume_ref, weights_ref, shear_ref, offsets_ref, measured_ref,
    columns_ref, spread_ref, residual_ref,
    slab, weights_in, shear, offsets, measured, sums, tiles, landed, measure_in, resid, pulls, pulled, resid_in,
    slab_sem, local_sem, out_sem, in_sem, back_out_sem, back_in_sem, m_out_sem, m_in_sem, r_out_sem, r_in_sem,
):
    slices = volume_ref.shape[0]
    angles = weights_ref.shape[0]
    owned = measured_ref.shape[0]
    base = (cols - owned) // 2
    count = rows * cols
    row, col = lax.axis_index("row"), lax.axis_index("col")
    me = row * cols + col
    at_home = jnp.logical_and(col >= base, col < base + owned)
    away = jnp.logical_not(at_home)
    mine = row * owned + lax.clamp(0, col - base, owned - 1)

    def home(angle):
        return angle // owned, base + lax.rem(angle, owned)

    unrolled = count <= UNROLL_UP_TO
    other_rows = [flip(row, step, rows) for step in reversed(range(rows))] if unrolled else None
    other_cols = [flip(col, step, cols) for step in far_first(cols)] if unrolled else None
    near = lax.clamp(0, col - base, owned - 1)
    other_places = [flip(near, step, owned) for step in far_first(owned)] if unrolled else None

    def peer(step):
        if unrolled:
            target = other_rows[step % rows], other_cols[step // rows]
            return target[0] * cols + target[1], target
        other = lax.rem(me + step + 1, count)
        return other, (other // cols, lax.rem(other, cols))

    def signal(device):
        pl.semaphore_signal(barrier, inc=1, device_id=device, device_id_type=MESH)

    barrier = pltpu.get_barrier_semaphore()

    @pl.when(at_home)
    def _():
        each(count - 1, lambda step: signal(peer(step)[1]))

    weights_copy = pltpu.make_async_copy(weights_ref, weights_in, local_sem.at[0])
    weights_copy.start()
    volume_copies = []
    for s in range(slices):
        copy = pltpu.make_async_copy(volume_ref.at[s], slab.at[s], slab_sem.at[s])
        copy.start()
        volume_copies.append(copy)
    shear_copy = pltpu.make_async_copy(shear_ref, shear, local_sem.at[1])
    shear_copy.start()
    measured_copy = pltpu.make_async_copy(measured_ref, measured, local_sem.at[2])
    measured_copy.start()
    offsets_copy = pltpu.make_async_copy(offsets_ref, offsets, local_sem.at[3])
    offsets_copy.start()

    @pl.when(away)
    def _():
        each(angles, lambda angle: signal(home(angle)))

    weights_copy.wait()
    weights = weights_in[...] * factor
    w_high, w_low = split(weights)
    w_both = jnp.concatenate([w_high, w_low], axis=0)
    for s in range(slices):
        volume_copies[s].wait()
        v_high, v_low = split(slab[s])
        first = jnp.dot(w_both, v_high, preferred_element_type=jnp.float32)
        second = jnp.dot(w_high, v_low, preferred_element_type=jnp.float32)
        sums[pl.ds(s, angles, stride=slices), :] = first[:angles] + first[angles:] + second
    shear_copy.wait()
    for a in range(angles):
        t_high, t_low = split(sums[a * slices:(a + 1) * slices, :])
        both = jnp.dot(jnp.concatenate([t_high, t_low], axis=0), shear[a], preferred_element_type=jnp.float32)
        tiles[a] = both[:slices] + both[slices:]
    measured_copy.wait()
    offsets_copy.wait()

    @pl.when(at_home)
    def _():
        pl.semaphore_wait(barrier, count - 1)

    @pl.when(away)
    def _():
        pl.semaphore_wait(barrier, angles)

    def send(source, target, send_sem, recv_sem, device):
        pltpu.make_async_remote_copy(
            src_ref=source, dst_ref=target, send_sem=send_sem, recv_sem=recv_sem,
            device_id=device, device_id_type=MESH).start()

    def send_measured(step):
        place = other_places[step] if unrolled else lax.rem(lax.select(at_home, col - base + 1, 0) + step, owned)
        send(measured.at[place], measure_in.at[col], m_out_sem, m_in_sem, (row, base + place))

    def send_tile(step):
        if unrolled:
            target, place = other_rows[step % rows], other_places[step // rows]
            send(tiles.at[target * owned + place], landed.at[me], out_sem, in_sem, (target, base + place))
            return
        angle = lax.rem(lax.select(at_home, mine + 1, row * owned) + step, angles)
        send(tiles.at[angle], landed.at[me], out_sem, in_sem, home(angle))

    each(owned - 1, send_measured)
    each(angles - 1, send_tile)

    @pl.when(away)
    def _():
        send_measured(owned - 1)
        send_tile(angles - 1)

    columns_ref[...] = jnp.concatenate(
        [weights, weights - w_high.astype(jnp.float32), weights], axis=0).T.astype(jnp.bfloat16)

    @pl.when(at_home)
    def _():
        landed[me] = tiles[mine]
        measure_in[col] = measured[col - base]
        offset = offsets[mine]
        bytes_of(measure_in, cols - 1, m_in_sem).wait()
        bytes_of(landed, count - 1, in_sem).wait()
        for c in range(cols):
            total = landed[c]
            for r in range(1, rows):
                total = total + landed[r * cols + lax.rem((cols - offset) * r + c, cols)]
            resid[c] = total - measure_in[c]
        for r in range(rows):
            for c in range(cols):
                pulls[r * cols + c] = resid[lax.rem(offset * r + c, cols)]

        def send_pull(step):
            other, device = peer(step)
            send(pulls.at[other], pulled.at[mine], back_out_sem, back_in_sem, device)

        def send_resid(step):
            other = other_cols[step] if unrolled else lax.rem(col + step + 1, cols)
            send(resid.at[other], resid_in.at[col - base], r_out_sem, r_in_sem, (row, other))

        each(count - 1, send_pull)
        each(cols - 1, send_resid)
        pulled[mine] = pulls[me]
        resid_in[col - base] = resid[col]
        bytes_of(pulled, angles - 1, back_in_sem).wait()

    @pl.when(away)
    def _():
        bytes_of(pulled, angles, back_in_sem).wait()

    for a in range(angles):
        p_high, p_low = split(pulled[a])
        both = lax.dot_general(
            jnp.concatenate([p_high, p_low], axis=0), shear[a], (((1,), (1,)), ((), ())),
            preferred_element_type=jnp.float32)
        sums[a * slices:(a + 1) * slices, :] = both[:slices] + both[slices:]
    for s in range(slices):
        g_high, g_low = split(sums[pl.ds(s, angles, stride=slices), :])
        spread_ref[s] = jnp.concatenate([g_high, g_high, g_low], axis=0)

    @pl.when(at_home)
    def _():
        bytes_of(resid_in, owned - 1, r_in_sem).wait()
        bytes_of(tiles, angles - 1, out_sem).wait()
        bytes_of(measured, owned - 1, m_out_sem).wait()
        bytes_of(pulls, count - 1, back_out_sem).wait()
        bytes_of(resid, cols - 1, r_out_sem).wait()

    @pl.when(away)
    def _():
        bytes_of(resid_in, owned, r_in_sem).wait()
        bytes_of(tiles, angles, out_sem).wait()
        bytes_of(measured, owned, m_out_sem).wait()

    residual_ref[...] = resid_in[...]


def finish(columns_ref, spread_ref, resid_ref, residual_ref, gradient_ref, stage, stage_sem, resid_sem):
    copies = [pltpu.make_async_copy(resid_ref, residual_ref, resid_sem)]
    copies[0].start()
    for s in range(spread_ref.shape[0]):
        stage[s] = jnp.dot(columns_ref[...], spread_ref[s], preferred_element_type=jnp.float32)
        copy = pltpu.make_async_copy(stage.at[s], gradient_ref.at[s], stage_sem.at[s])
        copy.start()
        copies.append(copy)
    for copy in copies:
        copy.wait()


def on_device(volume, ray_weights, shear_weights, shear_offsets, measured):
    rows, cols = lax.axis_size("row"), lax.axis_size("col")
    slices, slab_rows, width = volume.shape
    angles = ray_weights.shape[0]
    owned = measured.shape[0]
    count = rows * cols
    f32, bf16 = jnp.float32, jnp.bfloat16
    dma = pltpu.SemaphoreType.DMA
    vmem = pl.BlockSpec(memory_space=pltpu.VMEM)
    hbm = pl.BlockSpec(memory_space=pltpu.HBM)

    def blocks(number):
        return pltpu.VMEM((number, slices, width), f32)

    columns, spread, resid = pl.pallas_call(
        functools.partial(exchange, rows, cols, 1.0 / math.sqrt(slab_rows * rows)),
        out_shape=(
            jax.ShapeDtypeStruct((slab_rows, 3 * angles), bf16),
            jax.ShapeDtypeStruct((slices, 3 * angles, width), bf16),
            jax.ShapeDtypeStruct(measured.shape, f32)),
        in_specs=[hbm] * 5,
        out_specs=(vmem, vmem, vmem),
        scratch_shapes=[
            pltpu.VMEM(volume.shape, f32),
            pltpu.VMEM(ray_weights.shape, f32),
            pltpu.VMEM(shear_weights.shape, shear_weights.dtype),
            pltpu.SMEM(shear_offsets.shape, jnp.int32),
            blocks(owned),
            pltpu.VMEM((angles * slices, width), f32),
            blocks(angles), blocks(count), blocks(cols), blocks(cols), blocks(count), blocks(angles), blocks(owned),
            dma((slices,)), dma((4,)), dma, dma, dma, dma, dma, dma, dma, dma,
        ],
        compiler_params=pltpu.CompilerParams(collective_id=0, has_side_effects=True, vmem_limit_bytes=KERNEL_VMEM),
        name="exchange",
    )(*(pltpu.with_memory_space_constraint(value, pltpu.HBM)
        for value in (volume, ray_weights, shear_weights, shear_offsets, measured)))
    return pl.pallas_call(
        finish,
        out_shape=(jax.ShapeDtypeStruct(measured.shape, f32), jax.ShapeDtypeStruct(volume.shape, f32)),
        in_specs=[vmem] * 3,
        out_specs=(hbm, hbm),
        scratch_shapes=[pltpu.VMEM(volume.shape, f32), dma((slices,)), dma],
        compiler_params=pltpu.CompilerParams(vmem_limit_bytes=KERNEL_VMEM),
        name="finish",
    )(columns, spread, resid)


def solution(mesh):
    placed = (P(None, "row", "col"), P(None, "row"), P(), P(), P("row", None, "col"))
    return jax.shard_map(
        on_device,
        mesh=mesh,
        in_specs=placed,
        out_specs=(P("row", None, "col"), P(None, "row", "col")),
        check_vma=False,
    )
```

```python
import functools
import math

import jax
import jax.numpy as jnp
from jax import lax
from jax.experimental import pallas as pl
from jax.experimental.pallas import tpu as pltpu
from jax.sharding import PartitionSpec as P

MESH = pl.DeviceIdType.MESH
UNROLL_UP_TO = 64
KERNEL_VMEM = 24 * 1024 * 1024


def split(value):
    high = value.astype(jnp.bfloat16)
    return high, (value - high.astype(jnp.float32)).astype(jnp.bfloat16)


def each(count, body):
    if count <= UNROLL_UP_TO:
        for step in range(count):
            body(step)
    else:
        lax.fori_loop(0, count, lambda step, _: (body(step), 0)[1], 0)


def flip(index, step, size):
    if size & (size - 1):
        return lax.rem(index + step, size)
    bit = 1
    while bit < size:
        if step & bit:
            index = index + bit - 2 * bit * lax.rem(index // bit, 2)
        bit *= 2
    return index


def far_first(size):
    quarter = max(size // 4, 1)
    place = {2: 0, 3: 1, 1: 2, 0: 3}
    return sorted(range(size), key=lambda step: (place.get(step // quarter, 2), -step))


def bytes_of(ref, blocks, sem):
    part = ref.at[pl.ds(0, blocks)]
    return pltpu.make_async_copy(part, part, sem)


def exchange(
    rows, cols, factor,
    volume_ref, weights_ref, shear_ref, offsets_ref, measured_ref,
    columns_ref, spread_ref, residual_ref,
    slab, weights_in, shear, offsets, measured, sums, tiles, landed, measure_in, resid, pulls, pulled, resid_in,
    slab_sem, local_sem, out_sem, in_sem, back_out_sem, back_in_sem, m_out_sem, m_in_sem, r_out_sem, r_in_sem,
):
    slices = volume_ref.shape[0]
    angles = weights_ref.shape[0]
    owned = measured_ref.shape[0]
    base = (cols - owned) // 2
    count = rows * cols
    row, col = lax.axis_index("row"), lax.axis_index("col")
    me = row * cols + col
    at_home = jnp.logical_and(col >= base, col < base + owned)
    away = jnp.logical_not(at_home)
    mine = row * owned + lax.clamp(0, col - base, owned - 1)

    def home(angle):
        return angle // owned, base + lax.rem(angle, owned)

    unrolled = count <= UNROLL_UP_TO
    other_rows = [flip(row, step, rows) for step in reversed(range(rows))] if unrolled else None
    other_cols = [flip(col, step, cols) for step in far_first(cols)] if unrolled else None
    near = lax.clamp(0, col - base, owned - 1)
    other_places = [flip(near, step, owned) for step in far_first(owned)] if unrolled else None

    def peer(step):
        if unrolled:
            target = other_rows[step % rows], other_cols[step // rows]
            return target[0] * cols + target[1], target
        other = lax.rem(me + step + 1, count)
        return other, (other // cols, lax.rem(other, cols))

    def signal(device):
        pl.semaphore_signal(barrier, inc=1, device_id=device, device_id_type=MESH)

    barrier = pltpu.get_barrier_semaphore()

    @pl.when(at_home)
    def _():
        each(count - 1, lambda step: signal(peer(step)[1]))

    weights_copy = pltpu.make_async_copy(weights_ref, weights_in, local_sem.at[0])
    weights_copy.start()
    volume_copies = []
    for s in range(slices):
        copy = pltpu.make_async_copy(volume_ref.at[s], slab.at[s], slab_sem.at[s])
        copy.start()
        volume_copies.append(copy)
    shear_copy = pltpu.make_async_copy(shear_ref, shear, local_sem.at[1])
    shear_copy.start()
    measured_copy = pltpu.make_async_copy(measured_ref, measured, local_sem.at[2])
    measured_copy.start()
    offsets_copy = pltpu.make_async_copy(offsets_ref, offsets, local_sem.at[3])
    offsets_copy.start()

    @pl.when(away)
    def _():
        each(angles, lambda angle: signal(home(angle)))

    weights_copy.wait()
    weights = weights_in[...] * factor
    w_high, w_low = split(weights)
    w_both = jnp.concatenate([w_high, w_low], axis=0)
    for s in range(slices):
        volume_copies[s].wait()
        v_high, v_low = split(slab[s])
        first = jnp.dot(w_both, v_high, preferred_element_type=jnp.float32)
        second = jnp.dot(w_high, v_low, preferred_element_type=jnp.float32)
        sums[pl.ds(s, angles, stride=slices), :] = first[:angles] + first[angles:] + second
    shear_copy.wait()
    for a in range(angles):
        t_high, t_low = split(sums[a * slices:(a + 1) * slices, :])
        both = jnp.dot(jnp.concatenate([t_high, t_low], axis=0), shear[a], preferred_element_type=jnp.float32)
        tiles[a] = both[:slices] + both[slices:]
    measured_copy.wait()
    offsets_copy.wait()

    @pl.when(at_home)
    def _():
        pl.semaphore_wait(barrier, count - 1)

    @pl.when(away)
    def _():
        pl.semaphore_wait(barrier, angles)

    def send(source, target, send_sem, recv_sem, device):
        pltpu.make_async_remote_copy(
            src_ref=source, dst_ref=target, send_sem=send_sem, recv_sem=recv_sem,
            device_id=device, device_id_type=MESH).start()

    def send_measured(step):
        place = other_places[step] if unrolled else lax.rem(lax.select(at_home, col - base + 1, 0) + step, owned)
        send(measured.at[place], measure_in.at[col], m_out_sem, m_in_sem, (row, base + place))

    def send_tile(step):
        if unrolled:
            target, place = other_rows[step % rows], other_places[step // rows]
            send(tiles.at[target * owned + place], landed.at[me], out_sem, in_sem, (target, base + place))
            return
        angle = lax.rem(lax.select(at_home, mine + 1, row * owned) + step, angles)
        send(tiles.at[angle], landed.at[me], out_sem, in_sem, home(angle))

    each(angles - 1, send_tile)
    each(owned - 1, send_measured)

    @pl.when(away)
    def _():
        send_measured(owned - 1)
        send_tile(angles - 1)

    columns_ref[...] = jnp.concatenate(
        [weights, weights - w_high.astype(jnp.float32), weights], axis=0).T.astype(jnp.bfloat16)

    @pl.when(at_home)
    def _():
        landed[me] = tiles[mine]
        measure_in[col] = measured[col - base]
        offset = offsets[mine]
        bytes_of(measure_in, cols - 1, m_in_sem).wait()
        bytes_of(landed, count - 1, in_sem).wait()
        for c in range(cols):
            total = landed[c]
            for r in range(1, rows):
                total = total + landed[r * cols + lax.rem((cols - offset) * r + c, cols)]
            resid[c] = total - measure_in[c]
        for r in range(rows):
            for c in range(cols):
                pulls[r * cols + c] = resid[lax.rem(offset * r + c, cols)]

        def send_pull(step):
            other, device = peer(step)
            send(pulls.at[other], pulled.at[mine], back_out_sem, back_in_sem, device)

        def send_resid(step):
            other = other_cols[step] if unrolled else lax.rem(col + step + 1, cols)
            send(resid.at[other], resid_in.at[col - base], r_out_sem, r_in_sem, (row, other))

        each(count - 1, send_pull)
        each(cols - 1, send_resid)
        pulled[mine] = pulls[me]
        resid_in[col - base] = resid[col]
        bytes_of(pulled, angles - 1, back_in_sem).wait()

    @pl.when(away)
    def _():
        bytes_of(pulled, angles, back_in_sem).wait()

    for a in range(angles):
        p_high, p_low = split(pulled[a])
        both = lax.dot_general(
            jnp.concatenate([p_high, p_low], axis=0), shear[a], (((1,), (1,)), ((), ())),
            preferred_element_type=jnp.float32)
        sums[a * slices:(a + 1) * slices, :] = both[:slices] + both[slices:]
    for s in range(slices):
        g_high, g_low = split(sums[pl.ds(s, angles, stride=slices), :])
        spread_ref[s] = jnp.concatenate([g_high, g_high, g_low], axis=0)

    @pl.when(at_home)
    def _():
        bytes_of(resid_in, owned - 1, r_in_sem).wait()
        bytes_of(tiles, angles - 1, out_sem).wait()
        bytes_of(measured, owned - 1, m_out_sem).wait()
        bytes_of(pulls, count - 1, back_out_sem).wait()
        bytes_of(resid, cols - 1, r_out_sem).wait()

    @pl.when(away)
    def _():
        bytes_of(resid_in, owned, r_in_sem).wait()
        bytes_of(tiles, angles, out_sem).wait()
        bytes_of(measured, owned, m_out_sem).wait()

    residual_ref[...] = resid_in[...]


def finish(columns_ref, spread_ref, resid_ref, residual_ref, gradient_ref, stage, stage_sem, resid_sem):
    copies = [pltpu.make_async_copy(resid_ref, residual_ref, resid_sem)]
    copies[0].start()
    for s in range(spread_ref.shape[0]):
        stage[s] = jnp.dot(columns_ref[...], spread_ref[s], preferred_element_type=jnp.float32)
        copy = pltpu.make_async_copy(stage.at[s], gradient_ref.at[s], stage_sem.at[s])
        copy.start()
        copies.append(copy)
    for copy in copies:
        copy.wait()


def on_device(volume, ray_weights, shear_weights, shear_offsets, measured):
    rows, cols = lax.axis_size("row"), lax.axis_size("col")
    slices, slab_rows, width = volume.shape
    angles = ray_weights.shape[0]
    owned = measured.shape[0]
    count = rows * cols
    f32, bf16 = jnp.float32, jnp.bfloat16
    dma = pltpu.SemaphoreType.DMA
    vmem = pl.BlockSpec(memory_space=pltpu.VMEM)
    hbm = pl.BlockSpec(memory_space=pltpu.HBM)

    def blocks(number):
        return pltpu.VMEM((number, slices, width), f32)

    columns, spread, resid = pl.pallas_call(
        functools.partial(exchange, rows, cols, 1.0 / math.sqrt(slab_rows * rows)),
        out_shape=(
            jax.ShapeDtypeStruct((slab_rows, 3 * angles), bf16),
            jax.ShapeDtypeStruct((slices, 3 * angles, width), bf16),
            jax.ShapeDtypeStruct(measured.shape, f32)),
        in_specs=[hbm] * 5,
        out_specs=(vmem, vmem, vmem),
        scratch_shapes=[
            pltpu.VMEM(volume.shape, f32),
            pltpu.VMEM(ray_weights.shape, f32),
            pltpu.VMEM(shear_weights.shape, shear_weights.dtype),
            pltpu.SMEM(shear_offsets.shape, jnp.int32),
            blocks(owned),
            pltpu.VMEM((angles * slices, width), f32),
            blocks(angles), blocks(count), blocks(cols), blocks(cols), blocks(count), blocks(angles), blocks(owned),
            dma((slices,)), dma((4,)), dma, dma, dma, dma, dma, dma, dma, dma,
        ],
        compiler_params=pltpu.CompilerParams(collective_id=0, has_side_effects=True, vmem_limit_bytes=KERNEL_VMEM),
        name="exchange",
    )(*(pltpu.with_memory_space_constraint(value, pltpu.HBM)
        for value in (volume, ray_weights, shear_weights, shear_offsets, measured)))
    return pl.pallas_call(
        finish,
        out_shape=(jax.ShapeDtypeStruct(measured.shape, f32), jax.ShapeDtypeStruct(volume.shape, f32)),
        in_specs=[vmem] * 3,
        out_specs=(hbm, hbm),
        scratch_shapes=[pltpu.VMEM(volume.shape, f32), dma((slices,)), dma],
        compiler_params=pltpu.CompilerParams(vmem_limit_bytes=KERNEL_VMEM),
        name="finish",
    )(columns, spread, resid)


def solution(mesh):
    placed = (P(None, "row", "col"), P(None, "row"), P(), P(), P("row", None, "col"))
    return jax.shard_map(
        on_device,
        mesh=mesh,
        in_specs=placed,
        out_specs=(P("row", None, "col"), P(None, "row", "col")),
        check_vma=False,
    )
```
